32 devices in a mesh: groups: 2 (over x), freq: 8 (over z, y), gvec: 2 (over core).
Axes of the slice: x: 2, y: 2, z: 4, core: 2. Of those that a mesh axis runs over, the one named last changes fastest.
Arguments:
- screened: bfloat16 [16, 3072, 3072], P(('groups', 'freq'), 'gvec'), parts along dimension 0, may hold values from -0.109375 to 0.109375
- densities: bfloat16 [6144, 512], P(('groups', 'gvec'), 'freq'), parts along dimension 0, may hold values from -0.8046875 to 0.8046875
- pair_order: int32 [512], replicated, may hold values from 0 to 511, each once
- quad_index: int32 [4, 8], replicated, may hold values from 0 to 63
- quad_table: float32 [64], replicated, may hold values from 0.05 to 0.5
Outputs:
- kernel_out: float32 [8, 512, 512], P('groups', 'freq', 'gvec'), parts along dimension 0
The draws below stay inside these ranges and needn't reach their ends.
There are 2 independent parts, one for each index of `groups`. The reference program is written for one: setup_inputs(seed, part) draws one part's arguments, and reference() takes and returns one part's arrays. A program takes and returns all parts, laid end to end along the dimension named above; an argument that names none is the same for every part. Nothing has to cross between parts.
All inputs are finite; a program needn't handle non-finite values.
Results may differ from the reference program's by a relative error of at most 0.0029.
Values may be sent and summed in bfloat16 or wider, within the bound.
No kernel may reach another device: no remote copies, remote signals or barrier semaphores. Data moves between devices by JAX's collectives and lax.ppermute only.
A program may use at most 64 MiB of HBM per device.

```python
import math
import jax
import jax.numpy as jnp
from jax import lax

GVECS = 3072
PAIRS = 512
ENERGIES = 4
QUAD_ROWS = 64
FREQS = 8


def place_ends(values, key, least, top_value):
    longest = values.shape.index(max(values.shape))
    spots = []
    for shift in (0, 1):
        where = [jax.random.randint(jax.random.fold_in(key, axis), (), 0, length) for axis, length in enumerate(values.shape)]
        where[longest] = (where[longest] + shift) % values.shape[longest]
        spots.append(tuple(where))
    return values.at[spots[0]].set(least).at[spots[1]].set(top_value)


def block_scale(stream_key, extent, shards, low, largest):
    loudness, own = 1.0, jax.random.fold_in(stream_key, 6)
    for dim, blocks in shards:
        steps = jnp.exp(jax.random.uniform(jax.random.fold_in(own, dim), (blocks,), jnp.float32, low / len(shards), largest / len(shards)))
        loudness = loudness * jnp.repeat(steps, extent[dim] // blocks).reshape([-1 if axis == dim else 1 for axis in range(len(extent))])
    return loudness


def normal_values(own_key, extent, spread, reach, cuts=(), kind=jnp.bfloat16):
    entries = spread * jax.random.normal(own_key, extent, jnp.float32)
    if cuts:
        entries = entries * block_scale(own_key, extent, cuts, -0.22, 0.18)
    return jnp.clip(entries, -reach, reach).astype(kind)


def setup_inputs(seed: int = 0, part: int = 0) -> dict:
    key_list = jax.random.split(jax.random.key(seed), 6)
    part_splits = jax.random.split(jax.random.fold_in(key_list[5], part), 6)
    screened = normal_values(part_splits[0], (FREQS, GVECS, GVECS), GVECS ** -0.5, 0.109375, ((0, 8), (1, 2)))
    densities = normal_values(part_splits[1], (GVECS, PAIRS), (GVECS ** -0.25), 0.8046875, ((0, 2), (1, 8)))
    pair_order = jax.random.permutation(key_list[2], PAIRS).astype(jnp.int32)
    quad_index = place_ends(jax.random.randint(key_list[3], (ENERGIES, FREQS), 0, QUAD_ROWS), jax.random.fold_in(key_list[3], 1), 0, QUAD_ROWS - 1).astype(jnp.int32)
    quad_table = jnp.clip(jnp.exp(jax.random.uniform(key_list[4], (QUAD_ROWS,), jnp.float32, math.log(0.05), math.log(0.5))), 0.05, 0.5)
    return {"screened": screened, "densities": densities, "pair_order": pair_order, "quad_index": quad_index, "quad_table": quad_table}


def reference(screened, densities, pair_order, quad_index, quad_table):
    ordered = jnp.take(densities, pair_order, axis=1)
    weights = quad_table[quad_index]

    def advance(running, inputs):
        screen_now, weight_now = inputs
        product = jnp.dot(screen_now, ordered, preferred_element_type=jnp.float32).astype(jnp.bfloat16)
        kernel = jnp.dot(ordered.T, product, preferred_element_type=jnp.float32)
        return running + weight_now[:, None, None] * kernel, None

    start_value = jnp.zeros((ENERGIES, PAIRS, PAIRS), jnp.float32)
    running, unused = lax.scan(advance, start_value, (screened, weights.T))
    return running
```

```python
import jax
import jax.numpy as jnp
from jax import lax
from jax.sharding import PartitionSpec as P


def body(screened, densities, pair_order, quad_index, quad_table):
    freqs = lax.axis_size("freq")
    f = lax.axis_index("freq")
    h = lax.axis_index("gvec")
    screen = screened[0]
    half = densities.shape[0]
    own_pairs = densities.shape[1]
    pairs = own_pairs * freqs

    def shifted(x, d):
        return lax.ppermute(x, "freq", [(s, (s - d) % freqs) for s in range(freqs)])

    def sibling(x):
        return lax.ppermute(x, "gvec", [(0, 1), (1, 0)])

    own = densities.T
    chunks = [own] + [shifted(own, d) for d in range(1, freqs)]
    mine = jnp.concatenate(chunks, axis=0)
    other = sibling(mine)
    first = jnp.where(h == 0, mine, other)
    second = jnp.where(h == 0, other, mine)
    contract = (((1,), (1,)), ((), ()))
    product = lax.dot_general(
        screen, jnp.concatenate([first, second], axis=1), contract, preferred_element_type=jnp.float32
    ).astype(jnp.bfloat16)
    place = jnp.arange(pairs, dtype=jnp.int32)
    pair = (place + f * own_pairs) % pairs
    pick = (pair_order[:, None] == pair[None, :]).astype(jnp.bfloat16)
    rows = jnp.dot(pick, mine, preferred_element_type=jnp.float32).astype(jnp.bfloat16)
    cols = lax.dot_general(product, pick, contract, preferred_element_type=jnp.float32).astype(jnp.bfloat16)
    kernel = jnp.dot(rows, cols, preferred_element_type=jnp.float32)
    width = pairs // 2
    keep = lax.dynamic_slice_in_dim(kernel, h * width, width, axis=1)
    give = lax.dynamic_slice_in_dim(kernel, (1 - h) * width, width, axis=1)
    summed = keep + sibling(give)
    table_size = quad_table.shape[0]
    onehot = (
        quad_index[:, :, None] == jnp.arange(table_size, dtype=jnp.int32)[None, None, :]
    ).astype(jnp.float32)
    weights = jnp.sum(onehot * quad_table[None, None, :], axis=2)
    blocks = summed.reshape(freqs, own_pairs, width)
    out = None
    for d in range(freqs):
        block = lax.dynamic_index_in_dim(blocks, (f - d) % freqs, axis=0, keepdims=False)
        if d:
            block = shifted(block.astype(jnp.bfloat16), d).astype(jnp.float32)
        weight = lax.dynamic_index_in_dim(weights, (f + d) % freqs, axis=1, keepdims=False)
        term = weight[:, None, None] * block[None]
        out = term if out is None else out + term
    return out


def solution(mesh):
    placed = (P(("groups", "freq"), "gvec", None), P(("groups", "gvec"), "freq"), P(), P(), P())
    return jax.shard_map(
        body, mesh=mesh, in_specs=placed, out_specs=P("groups", "freq", "gvec"), check_vma=False
    )
```

```python
import jax
import jax.numpy as jnp
from jax import lax
from jax.experimental import pallas as pl
from jax.experimental.pallas import tpu as pltpu
from jax.sharding import PartitionSpec as P

LAST = (((1,), (1,)), ((), ()))


def dot(a, b):
    return jnp.dot(a, b, preferred_element_type=jnp.float32)


def dot_last(a, b):
    return lax.dot_general(a, b, LAST, preferred_element_type=jnp.float32)


def kernel_body(h_ref, w_mine, w_other, mine, other, rows, pick, out):
    step = pl.program_id(0)
    product = dot_last(w_mine[...], mine[...]) + dot_last(w_other[...], other[...])
    term = dot(rows[...], product.astype(jnp.bfloat16))

    @pl.when(step == 0)
    def _():
        out[...] = term

    @pl.when(step > 0)
    def _():
        out[...] += term

    @pl.when(step == pl.num_programs(0) - 1)
    def _():
        total = out[...]
        high = total.astype(jnp.bfloat16)
        low = (total - high.astype(jnp.float32)).astype(jnp.bfloat16)
        out[...] = dot_last(high, pick[...]) + dot_last(low, pick[...])


def contract(h, screen, mine, other, rows, pick):
    height, width = screen.shape
    half = width // 2
    pairs = mine.shape[0]
    block = next(b for b in (256, 128, 64, 32, 16, 8) if height % b == 0)
    whole = lambda i, h: (0, 0)
    return pl.pallas_call(
        kernel_body,
        grid_spec=pltpu.PrefetchScalarGridSpec(
            num_scalar_prefetch=1,
            grid=(height // block,),
            in_specs=[
                pl.BlockSpec((block, half), lambda i, h: (i, h[0])),
                pl.BlockSpec((block, half), lambda i, h: (i, 1 - h[0])),
                pl.BlockSpec((pairs, half), whole),
                pl.BlockSpec((pairs, half), whole),
                pl.BlockSpec((pairs, block), lambda i, h: (0, i)),
                pl.BlockSpec((pairs, pairs), whole),
            ],
            out_specs=pl.BlockSpec((pairs, pairs), whole),
        ),
        out_shape=jax.ShapeDtypeStruct((pairs, pairs), jnp.float32),
        compiler_params=pltpu.CompilerParams(dimension_semantics=("arbitrary",)),
    )(h.reshape(1), screen, screen, mine, other, rows, pick)


def body(screened, densities, pair_order, quad_index, quad_table):
    freqs = lax.axis_size("freq")
    outer = freqs // 2
    f = lax.axis_index("freq")
    h = lax.axis_index("gvec")
    z, y = f // 2, f % 2
    screen = screened[0]
    own_pairs = densities.shape[1]
    pairs = own_pairs * freqs

    def swapped(x, k):
        return lax.ppermute(x, "freq", [(s, s ^ k) for s in range(freqs)])

    def sibling(x):
        return lax.ppermute(x, "gvec", [(0, 1), (1, 0)])

    own = densities.T
    far = [swapped(own, 2 * k) for k in range(outer - 1, 0, -1)][::-1]
    chunks = []
    for chunk in [own] + far:
        chunks += [chunk, swapped(chunk, 1)]
    mine = jnp.concatenate(chunks, axis=0)
    other = sibling(mine)
    place = jnp.arange(pairs, dtype=jnp.int32)
    pair = ((place // own_pairs) ^ f) * own_pairs + place % own_pairs
    pick = (pair_order[:, None] == pair[None, :]).astype(jnp.bfloat16)
    rows = dot(pick, mine).astype(jnp.bfloat16)
    kernel = contract(h, screen, mine, other, rows, pick)

    blocks = kernel.reshape(outer, 2, own_pairs, pairs)
    keep = lax.dynamic_index_in_dim(blocks, h, axis=1, keepdims=False)
    give = lax.dynamic_index_in_dim(blocks, 1 - h, axis=1, keepdims=False)
    summed = (keep + sibling(give)).astype(jnp.bfloat16)

    onehot = (
        quad_index[:, :, None] == jnp.arange(quad_table.shape[0], dtype=jnp.int32)[None, None, :]
    ).astype(jnp.float32)
    weights = jnp.sum(onehot * quad_table[None, None, :], axis=2)
    partial = None
    for k in range(outer - 1, -1, -1):
        route = []
        for s in range(outer):
            for t in range(2):
                for c in range(2):
                    route.append(((s * 2 + t) * 2 + c, ((s ^ k) * 2 + c) * 2 + (t ^ c)))
        block = lax.dynamic_index_in_dim(summed, z ^ k, axis=0, keepdims=False)
        block = lax.ppermute(block, ("freq", "gvec"), route).astype(jnp.float32)
        weight = lax.dynamic_index_in_dim(weights, f ^ (2 * k + h), axis=1, keepdims=False)
        term = weight[:, None, None] * block[None]
        partial = term if partial is None else partial + term
    width = pairs // 2
    keep = lax.dynamic_slice_in_dim(partial, h * width, width, axis=2)
    give = lax.dynamic_slice_in_dim(partial, (1 - h) * width, width, axis=2)
    return keep + sibling(give)


def solution(mesh):
    placed = (P(("groups", "freq"), "gvec", None), P(("groups", "gvec"), "freq"), P(), P(), P())
    return jax.shard_map(
        body, mesh=mesh, in_specs=placed, out_specs=P("groups", "freq", "gvec"), check_vma=False
    )
```

```python
import jax
import jax.numpy as jnp
from jax import lax
from jax.experimental import pallas as pl
from jax.experimental.pallas import tpu as pltpu
from jax.sharding import PartitionSpec as P

LAST = (((1,), (1,)), ((), ()))


def dot(a, b):
    return jnp.dot(a, b, preferred_element_type=jnp.float32)


def dot_last(a, b):
    return lax.dot_general(a, b, LAST, preferred_element_type=jnp.float32)


def first_body(where, w_mine, w_other, mine, other, out):
    product = dot_last(w_mine[...], mine[...]) + dot_last(w_other[...], other[...])
    out[...] = product.astype(jnp.bfloat16)


def split(x):
    high = x.astype(jnp.bfloat16)
    return high, (x - high.astype(jnp.float32)).astype(jnp.bfloat16)


def second_body(where, w_mine, w_other, mine, other, early, left0, left1, order, pair, keep, give, acc):
    step = pl.program_id(0)
    half = mine.shape[0]
    product = dot_last(w_mine[...], mine[...]) + dot_last(w_other[...], other[...])
    product = product.astype(jnp.bfloat16)

    @pl.when(step == 0)
    def _():
        acc[...] = jnp.zeros_like(acc)

    for n, left in enumerate((left0, left1)):
        rows = pl.ds(n * half, half)
        acc[rows, :half] += dot(left[...], early[...])
        acc[rows, half:] += dot(left[...], product)

    @pl.when(step == pl.num_programs(0) - 1)
    def _():
        pick = jnp.where(order[...] == pair[...], 1.0, 0.0).astype(jnp.bfloat16)
        high, low = split(acc[...])
        high, low = split(dot_last(high, pick) + dot_last(low, pick))
        acc[...] = dot(pick, high) + dot(pick, low)
        outer = keep.shape[0]
        own = keep.shape[1]
        f, h = where[0], where[1]
        for k in range(outer):
            chip = (f // 2) ^ k
            keep[k] = acc[pl.ds(pl.multiple_of((chip * 2 + h) * own, own), own), :]
            give[k] = acc[pl.ds(pl.multiple_of((chip * 2 + 1 - h) * own, own), own), :]


def fixed(*shape):
    return pl.BlockSpec(shape, lambda i, where: (0,) * len(shape))


def row_block(height):
    return next(b for b in (256, 128, 64, 32, 16, 8) if height % b == 0)


def screen_specs(block, half):
    return [
        pl.BlockSpec((block, half), lambda i, where: (i, where[1])),
        pl.BlockSpec((block, half), lambda i, where: (i, 1 - where[1])),
    ]


def first_product(where, screen, mine, other):
    height, width = screen.shape
    some, half = mine.shape
    block = row_block(height)
    return pl.pallas_call(
        first_body,
        grid_spec=pltpu.PrefetchScalarGridSpec(
            num_scalar_prefetch=1,
            grid=(height // block,),
            in_specs=screen_specs(block, half) + [fixed(some, half), fixed(some, half)],
            out_specs=pl.BlockSpec((block, some), lambda i, where: (i, 0)),
        ),
        out_shape=jax.ShapeDtypeStruct((height, some), jnp.bfloat16),
        compiler_params=pltpu.CompilerParams(dimension_semantics=("arbitrary",)),
    )(where, screen, screen, mine, other)


def second_product(where, screen, mine, other, early, left0, order, pair, outer):
    height, width = screen.shape
    some, half = mine.shape
    pairs = 2 * some
    own = pairs // (2 * outer)
    block = row_block(height)
    left = pl.BlockSpec((some, block), lambda i, where: (0, i))
    shape = (outer, own, pairs)
    return pl.pallas_call(
        second_body,
        grid_spec=pltpu.PrefetchScalarGridSpec(
            num_scalar_prefetch=1,
            grid=(height // block,),
            in_specs=screen_specs(block, half)
            + [
                fixed(some, half),
                fixed(some, half),
                pl.BlockSpec((block, some), lambda i, where: (i, 0)),
                left,
                left,
                fixed(pairs, 1),
                fixed(1, pairs),
            ],
            out_specs=[fixed(*shape), fixed(*shape)],
            scratch_shapes=[pltpu.VMEM((pairs, pairs), jnp.float32)],
        ),
        out_shape=[jax.ShapeDtypeStruct(shape, jnp.float32)] * 2,
        compiler_params=pltpu.CompilerParams(dimension_semantics=("arbitrary",)),
    )(where, screen, screen, mine, other, early, left0, mine, order.reshape(pairs, 1), pair.reshape(1, pairs))


def body(screened, densities, pair_order, quad_index, quad_table):
    freqs = lax.axis_size("freq")
    outer = freqs // 2
    f = lax.axis_index("freq")
    h = lax.axis_index("gvec")
    screen = screened[0]
    own_pairs = densities.shape[1]
    pairs = own_pairs * freqs

    def swapped(x, k):
        return lax.ppermute(x, "freq", [(s, s ^ k) for s in range(freqs)])

    def sibling(x):
        return lax.ppermute(x, "gvec", [(0, 1), (1, 0)])

    own = densities.T
    far = {k: swapped(own, 2 * k) for k in range(outer - 1, 0, -1)}
    far[0] = own
    near = range((outer + 1) // 2)
    late = range((outer + 1) // 2, outer)

    def gathered(some):
        parts = []
        for k in some:
            parts += [far[k], swapped(far[k], 1)]
        return jnp.concatenate(parts, axis=0)

    where = jnp.stack([f, h]).astype(jnp.int32)
    mine0 = gathered(near)
    early = first_product(where, screen, mine0, sibling(mine0))
    held = lax.optimization_barrier([early] + [far[k] for k in late])
    early = held[0]
    for k, chunk in zip(late, held[1:]):
        far[k] = chunk
    mine1 = gathered(late)
    place = jnp.arange(pairs, dtype=jnp.int32)
    pair = ((place // own_pairs) ^ f) * own_pairs + place % own_pairs
    keep, give = second_product(
        where, screen, mine1, sibling(mine1), early, mine0, pair_order, pair, outer
    )
    summed = (keep + sibling(give)).astype(jnp.bfloat16)

    onehot = (
        quad_index[:, :, None] == jnp.arange(quad_table.shape[0], dtype=jnp.int32)[None, None, :]
    ).astype(jnp.float32)
    weights = jnp.sum(onehot * quad_table[None, None, :], axis=2)
    partial = None
    for k in range(outer - 1, -1, -1):
        route = []
        for s in range(outer):
            for t in range(2):
                for c in range(2):
                    route.append(((s * 2 + t) * 2 + c, ((s ^ k) * 2 + c) * 2 + (t ^ c)))
        block = lax.ppermute(summed[k], ("freq", "gvec"), route).astype(jnp.float32)
        weight = lax.dynamic_index_in_dim(weights, f ^ (2 * k + h), axis=1, keepdims=False)
        term = weight[:, None, None] * block[None]
        partial = term if partial is None else partial + term
    width = pairs // 2
    keep = lax.dynamic_slice_in_dim(partial, h * width, width, axis=2)
    give = lax.dynamic_slice_in_dim(partial, (1 - h) * width, width, axis=2)
    return keep + sibling(give)


def solution(mesh):
    placed = (P(("groups", "freq"), "gvec", None), P(("groups", "gvec"), "freq"), P(), P(), P())
    return jax.shard_map(
        body, mesh=mesh, in_specs=placed, out_specs=P("groups", "freq", "gvec"), check_vma=False
    )
```

```python
import jax
import jax.numpy as jnp
from jax import lax
from jax.experimental import pallas as pl
from jax.experimental.pallas import tpu as pltpu
from jax.sharding import PartitionSpec as P

LAST = (((1,), (1,)), ((), ()))


def dot(a, b):
    return jnp.dot(a, b, preferred_element_type=jnp.float32)


def dot_last(a, b):
    return lax.dot_general(a, b, LAST, preferred_element_type=jnp.float32)


def dot_first(a, b):
    return lax.dot_general(a, b, (((0,), (0,)), ((), ())), preferred_element_type=jnp.float32)


def split(x):
    high = x.astype(jnp.bfloat16)
    return high, (x - high.astype(jnp.float32)).astype(jnp.bfloat16)


def kernel_body(where, w_mine, w_other, mine, other, left, order, keep, give, acc):
    step = pl.program_id(0)
    outer, own, pairs = keep.shape
    f, h = where[0], where[1]
    product = dot_last(w_mine[...], mine[...]) + dot_last(w_other[...], other[...])
    term = dot(left[...], product.astype(jnp.bfloat16))

    @pl.when(step == 0)
    def _():
        acc[...] = term

    @pl.when(step > 0)
    def _():
        acc[...] += term

    @pl.when(step == pl.num_programs(0) - 1)
    def _():
        place = lax.broadcasted_iota(jnp.int32, (pairs, pairs), 0)
        pair = ((place // own) ^ f) * own + place % own
        pick = jnp.where(pair == order[...], 1.0, 0.0).astype(jnp.bfloat16)
        high, low = split(acc[...])
        high, low = split(dot(high, pick) + dot(low, pick))
        acc[...] = dot_first(pick, high) + dot_first(pick, low)
        for k in range(outer):
            chip = (f // 2) ^ k
            keep[k] = acc[pl.ds(pl.multiple_of((chip * 2 + h) * own, own), own), :]
            give[k] = acc[pl.ds(pl.multiple_of((chip * 2 + 1 - h) * own, own), own), :]


def contract(where, screen, mine, other, order, outer, most=256):
    height, width = screen.shape
    pairs, half = mine.shape
    own = pairs // (2 * outer)
    block = next(b for b in (most, 256, 128, 64, 32, 16, 8) if height % b == 0)
    fixed = lambda *shape: pl.BlockSpec(shape, lambda i, where: (0,) * len(shape))
    shape = (outer, own, pairs)
    return pl.pallas_call(
        kernel_body,
        grid_spec=pltpu.PrefetchScalarGridSpec(
            num_scalar_prefetch=1,
            grid=(height // block,),
            in_specs=[
                pl.BlockSpec((block, half), lambda i, where: (i, where[1])),
                pl.BlockSpec((block, half), lambda i, where: (i, 1 - where[1])),
                fixed(pairs, half),
                fixed(pairs, half),
                pl.BlockSpec((pairs, block), lambda i, where: (0, i)),
                fixed(1, pairs),
            ],
            out_specs=[fixed(*shape), fixed(*shape)],
            scratch_shapes=[pltpu.VMEM((pairs, pairs), jnp.float32)],
        ),
        out_shape=[jax.ShapeDtypeStruct(shape, jnp.float32)] * 2,
        compiler_params=pltpu.CompilerParams(dimension_semantics=("arbitrary",)),
    )(where, screen, screen, mine, other, mine, order.reshape(1, pairs))


def body(screened, densities, pair_order, quad_index, quad_table):
    freqs = lax.axis_size("freq")
    outer = freqs // 2
    f = lax.axis_index("freq")
    h = lax.axis_index("gvec")
    screen = screened[0]
    own_pairs = densities.shape[1]
    pairs = own_pairs * freqs

    def swapped(x, k):
        return lax.ppermute(x, "freq", [(s, s ^ k) for s in range(freqs)])

    def sibling(x):
        return lax.ppermute(x, "gvec", [(0, 1), (1, 0)])

    own = densities.T
    far = [swapped(own, 2 * k) for k in range(outer - 1, 0, -1)][::-1]
    chunks = []
    for chunk in [own] + far:
        chunks += [chunk, swapped(chunk, 1)]
    mine = jnp.concatenate(chunks, axis=0)
    where = jnp.stack([f, h]).astype(jnp.int32)
    keep, give = contract(where, screen, mine, sibling(mine), pair_order, outer)
    summed = (keep + sibling(give)).astype(jnp.bfloat16)

    onehot = (
        quad_index[:, :, None] == jnp.arange(quad_table.shape[0], dtype=jnp.int32)[None, None, :]
    ).astype(jnp.float32)
    weights = jnp.sum(onehot * quad_table[None, None, :], axis=2)
    partial = None
    for k in range(outer - 1, -1, -1):
        route = []
        for s in range(outer):
            for t in range(2):
                for c in range(2):
                    route.append(((s * 2 + t) * 2 + c, ((s ^ k) * 2 + c) * 2 + (t ^ c)))
        block = lax.ppermute(summed[k], ("freq", "gvec"), route).astype(jnp.float32)
        weight = lax.dynamic_index_in_dim(weights, f ^ (2 * k + h), axis=1, keepdims=False)
        term = weight[:, None, None] * block[None]
        partial = term if partial is None else partial + term
    width = pairs // 2
    keep = lax.dynamic_slice_in_dim(partial, h * width, width, axis=2)
    give = lax.dynamic_slice_in_dim(partial, (1 - h) * width, width, axis=2)
    return keep + sibling(give)


def solution(mesh):
    placed = (P(("groups", "freq"), "gvec", None), P(("groups", "gvec"), "freq"), P(), P(), P())
    return jax.shard_map(
        body, mesh=mesh, in_specs=placed, out_specs=P("groups", "freq", "gvec"), check_vma=False
    )
```
